256 devices in a mesh: gx: 8 (over y, x_hi), gy: 4 (over x_lo, core), gz: 8 (over z).
Axes of the slice: x: 4 (x_hi: 2, x_lo: 2; x = x_hi * 2 + x_lo), y: 4, z: 8, core: 2. Of those that a mesh axis runs over, the one named last changes fastest.
Arguments:
- source: bfloat16 [512, 512, 512], P('gz', 'gx', 'gy'), may hold values from -6 to 6
- forward_x: bfloat16 [512, 512], replicated, may hold values from -0.25 to 0.25
- forward_y: bfloat16 [512, 512], replicated, may hold values from -0.25 to 0.25
- forward_z: bfloat16 [512, 512], replicated, may hold values from -0.25 to 0.25
- inverse_x: bfloat16 [512, 512], replicated, may hold values from -0.25 to 0.25
- inverse_y: bfloat16 [512, 512], replicated, may hold values from -0.25 to 0.25
- inverse_z: bfloat16 [512, 512], replicated, may hold values from -0.25 to 0.25
- values_x: float32 [512], replicated, may hold values from 0.1 to 2
- values_y: float32 [512], replicated, may hold values from 0.1 to 2
- values_z: float32 [512], replicated, may hold values from 0.1 to 2
Outputs:
- solution: bfloat16 [512, 512, 512], P('gz', 'gx', 'gy')
The draws below stay inside these ranges and needn't reach their ends.
All inputs are finite; a program needn't handle non-finite values.
Results may differ from the reference program's by a relative error of at most 0.015.
Values may be sent and summed in bfloat16 or wider, within the bound.
A program may use at most 64 MiB of HBM per device.

```python
import math
import jax
import jax.numpy as jnp
from jax import lax

NX = 512
NY = 512
NZ = 512


def block_levels(rng, shape, cuts, least, high):
    def one(dim, blocks):
        steps = jax.random.uniform(jax.random.fold_in(jax.random.fold_in(rng, 6), dim), (blocks,), jnp.float32, least / len(cuts), high / len(cuts))
        return jnp.repeat(jnp.exp(steps), shape[dim] // blocks).reshape((-1,) + (1,) * (len(shape) - dim - 1))

    loudness = one(*cuts[0])
    for cut in cuts[1:]:
        loudness = loudness * one(*cut)
    return loudness


def scatter_about(own_key, dims, deviation, most, pieces=(), kind=jnp.bfloat16):
    loudness = block_levels(own_key, dims, pieces, -0.22, 0.18) if pieces else 1.0
    drawn = jax.random.normal(own_key, dims, jnp.float32) * deviation * loudness
    return jnp.minimum(jnp.maximum(drawn, -most), most).astype(kind)


def setup_inputs(seed: int = 0) -> dict:
    streams_of = jax.random.split(jax.random.key(seed), 11)
    source = scatter_about(streams_of[0], (NZ, NY, NX), 1.0, 6.0, ((0, 8), (1, 8), (2, 4)))
    forward_x = scatter_about(streams_of[1], (NX, NX), NX ** -0.5, 0.25)
    forward_y = scatter_about(streams_of[2], (NY, NY), NY ** -0.5, 0.25)
    forward_z = scatter_about(streams_of[3], (NZ, NZ), NZ ** -0.5, 0.25)
    inverse_x = scatter_about(streams_of[4], (NX, NX), NX ** -0.5, 0.25)
    inverse_y = scatter_about(streams_of[5], (NY, NY), NY ** -0.5, 0.25)
    inverse_z = scatter_about(streams_of[6], (NZ, NZ), NZ ** -0.5, 0.25)
    values_x = jnp.clip(jnp.exp(jax.random.uniform(streams_of[7], (NX,), jnp.float32, math.log(0.1), math.log(2.0))), 0.1, 2.0)
    values_y = jnp.clip(jnp.exp(jax.random.uniform(streams_of[8], (NY,), jnp.float32, math.log(0.1), math.log(2.0))), 0.1, 2.0)
    values_z = jnp.clip(jnp.exp(jax.random.uniform(streams_of[9], (NZ,), jnp.float32, math.log(0.1), math.log(2.0))), 0.1, 2.0)
    return {"source": source, "forward_x": forward_x, "forward_y": forward_y, "forward_z": forward_z, "inverse_x": inverse_x, "inverse_y": inverse_y, "inverse_z": inverse_z, "values_x": values_x, "values_y": values_y, "values_z": values_z}


def along_x(data, basis):
    depth, rows, cols = data.shape
    flat = data.reshape(depth * rows, cols)
    out = jnp.dot(flat, basis.T, preferred_element_type=jnp.float32)
    return out.astype(jnp.bfloat16).reshape(depth, rows, basis.shape[0])


def along_y(data, basis):
    def single(plane):
        return jnp.dot(basis, plane, preferred_element_type=jnp.float32).astype(jnp.bfloat16)
    return lax.map(single, data)


def along_z(data, basis):
    depth, rows, cols = data.shape
    out = jnp.dot(basis, data.reshape(depth, rows * cols), preferred_element_type=jnp.float32)
    return out.astype(jnp.bfloat16).reshape(basis.shape[0], rows, cols)


def reference(source, forward_x, forward_y, forward_z, inverse_x, inverse_y, inverse_z, values_x, values_y, values_z):
    step_a = along_x(source, forward_x)
    step_b = along_y(step_a, forward_y)
    step_c = along_z(step_b, forward_z)
    denom = values_z[:, None, None] + values_y[None, :, None] + values_x[None, None, :]
    scaled = (step_c.astype(jnp.float32) / denom).astype(jnp.bfloat16)
    step_d = along_z(scaled, inverse_z)
    step_e = along_y(step_d, inverse_y)
    return along_x(step_e, inverse_x)
```

```python
import functools

import jax
import jax.numpy as jnp
from jax import lax
from jax.experimental import pallas as pl
from jax.experimental.pallas import tpu as pltpu
from jax.sharding import PartitionSpec as P

MESH = pl.DeviceIdType.MESH
F32 = jnp.float32
BF16 = jnp.bfloat16
NX, NY, NZ = 8, 4, 8
N = 512
K = 4
PITCH = N + 8
OPITCH = 128 + 8
FAR_FIRST = (4, 3, 5, 2, 6, 1, 7)


def dot(a, b):
    return jnp.dot(a, b, preferred_element_type=F32)


def dot_t(a, b):
    return lax.dot_general(a, b, (((1,), (1,)), ((), ())), preferred_element_type=F32)


def kernel(
    src, fx, fy, fz, ix, iy, iz, vx, vy, vz, out,
    xin, psend, ybuf, yout, zbuf, zlines, recip, scaled, olines, zsend, ybuf2, yout2, pbuf, xg, xout,
    weights, izp, vxs, vys, vzs, recv, send, wsem, vsem, lsem,
):
    gx, gy, gz = lax.axis_index("gx"), lax.axis_index("gy"), lax.axis_index("gz")
    me = gz * NY + gy

    def dev(a, b, c):
        return {"gx": a, "gy": b, "gz": c}

    def remote(s, d, stage, k, where):
        pltpu.make_async_remote_copy(
            src_ref=s, dst_ref=d, send_sem=send.at[stage], recv_sem=recv.at[stage, k],
            device_id=where, device_id_type=MESH,
        ).start()

    def arrived(ref, sem):
        pltpu.make_async_copy(ref, ref, sem).wait()

    barrier = pltpu.get_barrier_semaphore()
    for d in range(1, NX):
        pl.semaphore_signal(barrier, inc=1, device_id=dev(lax.rem(gx + d, NX), gy, gz), device_id_type=MESH)
    for c in range(NZ):
        for b in range(NY):
            if b or c:
                pl.semaphore_signal(
                    barrier, inc=1, device_id=dev(gx, lax.rem(gy + b, NY), lax.rem(gz + c, NZ)), device_id_type=MESH
                )

    for k in range(K):
        pltpu.make_async_copy(
            src.at[pl.ds(16 * gy + 4 * k, 4)],
            xin.at[k, :, :, pl.ds(pl.multiple_of(128 * gy, 128), 128)],
            recv.at[0, k],
        ).start()
    loads = [pltpu.make_async_copy(w, weights.at[i], wsem.at[i]) for i, w in enumerate((fx, fy, fz, iz, iy, ix))]
    for c in loads:
        c.start()
    vloads = [pltpu.make_async_copy(v, s, vsem.at[i]) for i, (v, s) in enumerate(((vx, vxs), (vy, vys), (vz, vzs)))]
    for c in vloads:
        c.start()

    pl.semaphore_wait(barrier, NX - 1 + NZ * NY - 1)

    for k in range(K):
        for d in range(1, NY):
            to = lax.rem(gy + d, NY)
            remote(
                src.at[pl.ds(16 * to + 4 * k, 4)],
                xin.at[k, :, :, pl.ds(pl.multiple_of(128 * gy, 128), 128)],
                0, k, dev(gx, to, gz),
            )

    lane = lax.broadcasted_iota(jnp.int32, (8, 128), 1)
    sub = lax.broadcasted_iota(jnp.int32, (8, 128), 0)
    low = lane < 64

    def exchange_halves(a, b):
        keep = jnp.broadcast_to(lax.broadcasted_iota(jnp.int32, (1, 128), 1) < 64, a.shape)
        return (
            jnp.where(keep, a, pltpu.roll(b, 64, 1)),
            jnp.where(keep, pltpu.roll(a, 64, 1), b),
        )

    for c in vloads:
        c.wait()
    along_p = jnp.zeros((8, 128), F32)
    for i in range(64):
        along_p = jnp.where((lane & 63) == i, vxs[64 * gx + i], along_p)
    along_qp = [
        along_p + jnp.where(low, vys[16 * me + q], vys[16 * me + q + 8]) for q in range(8)
    ]

    def reciprocals(g, _):
        col = jnp.zeros((8, 128), F32)
        for i in range(8):
            col = jnp.where(sub == i, vzs[8 * g + i], col)
        rows = pl.ds(pl.multiple_of(8 * g, 8), 8)
        for q in range(8):
            recip[rows, 128 * q : 128 * (q + 1)] = 1.0 / (col + along_qp[q])
        return 0

    lax.fori_loop(0, N // 8, reciprocals, 0)

    loads[3].wait()
    row = lax.broadcasted_iota(jnp.int32, (N, N), 0)
    wanted = ((row & 127) >> 2) * 16 + (row >> 7) * 4 + (row & 3)
    order = (lax.broadcasted_iota(jnp.int32, (N, N), 1) == wanted).astype(F32).astype(BF16)
    izp[...] = dot(order, weights[3]).astype(BF16)

    def forward_x(k):
        arrived(xin.at[k], recv.at[0, k])
        o = dot_t(xin[k].reshape(256, N), weights[0]).reshape(2, 2, 64, N)
        for zp in range(2):
            for t in range(4):
                a, b = exchange_halves(o[zp, 0, :, 128 * t : 128 * (t + 1)], o[zp, 1, :, 128 * t : 128 * (t + 1)])
                psend[k, 2 * t, zp] = a.astype(BF16)
                psend[k, 2 * t + 1, zp] = b.astype(BF16)
        rows = pl.ds(pl.multiple_of(64 * gx, 64), 64)
        for d in range(1, NX):
            to = lax.rem(gx + d, NX)
            remote(psend.at[k, to], ybuf.at[k, :, rows, :], 1, k, dev(to, gy, gz))
        for zp in range(2):
            ybuf[k, zp, rows, :] = psend[k, gx, zp]

    def forward_y(k):
        arrived(psend.at[k, 0:7], recv.at[1, k])
        o = dot(weights[1], jnp.concatenate([ybuf[k, 0], ybuf[k, 1]], axis=1))
        for zp in range(2):
            yout[k, zp] = o[:, 128 * zp : 128 * (zp + 1)].astype(BF16)

        def to_lines(b, c):
            to_b, to_c = lax.rem(gy + b, NY), lax.rem(gz + c, NZ)
            rows = pl.ds(pl.multiple_of(16 * (to_c * NY + to_b), 16), 16)
            remote(yout.at[k, :, rows, :], zbuf.at[k, me], 2, k, dev(gx, to_b, to_c))

        for c in FAR_FIRST:
            lax.fori_loop(0, NY, lambda b, _, c=c: (to_lines(b, c), 0)[1], 0)
        lax.fori_loop(1, NY, lambda b, _: (to_lines(b, 0), 0)[1], 0)
        rows = pl.ds(pl.multiple_of(16 * me, 16), 16)
        for zp in range(2):
            zbuf[k, me, zp] = yout[k, zp, rows, :]

    def to_z_rows(k):
        arrived(zbuf.at[k, 0:31], recv.at[2, k])

        def some(g, _):
            for s in range(8):
                for zp in range(2):
                    tile = zbuf[k, 8 * g + s, zp].astype(F32)
                    a, b = exchange_halves(tile[:8], tile[8:])
                    z = 16 * (8 * g + s) + 4 * k + 2 * zp
                    zlines[pl.ds(z, 8, stride=PITCH), :] = a
                    zlines[pl.ds(z + 1, 8, stride=PITCH), :] = b
            return 0

        lax.fori_loop(0, 4, some, 0)

    def along_z():
        for h in range(4):
            d = jnp.concatenate(
                [zlines[PITCH * q : PITCH * q + N, :] for q in (2 * h, 2 * h + 1)], axis=1
            ).astype(BF16)
            c = dot(weights[2], d).astype(BF16).astype(F32)
            scaled[:, 256 * h : 256 * (h + 1)] = (c * recip[:, 256 * h : 256 * (h + 1)]).astype(BF16)

    def from_z_rows(k):
        for h in range(4):
            o = dot(izp[128 * k : 128 * (k + 1), :], scaled[:, 256 * h : 256 * (h + 1)])
            for j in range(2):
                q = 2 * h + j
                olines[k, OPITCH * q : OPITCH * q + 128, :] = o[:, 128 * j : 128 * (j + 1)]

        def some(g, _):
            for s in range(8):
                for zp in range(2):
                    at = 4 * (8 * g + s) + 2 * zp
                    a, b = exchange_halves(
                        olines[k, pl.ds(at, 8, stride=OPITCH), :], olines[k, pl.ds(at + 1, 8, stride=OPITCH), :]
                    )
                    zsend[k, 8 * g + s, zp] = jnp.concatenate([a, b], axis=0).astype(BF16)
            return 0

        lax.fori_loop(0, 4, some, 0)
        rows = pl.ds(pl.multiple_of(16 * me, 16), 16)

        def to_planes(b, c):
            to_b, to_c = lax.rem(gy + b, NY), lax.rem(gz + c, NZ)
            remote(zsend.at[k, to_c * NY + to_b], ybuf2.at[k, :, rows, :], 3, k, dev(gx, to_b, to_c))

        for c in FAR_FIRST:
            lax.fori_loop(0, NY, lambda b, _, c=c: (to_planes(b, c), 0)[1], 0)
        lax.fori_loop(1, NY, lambda b, _: (to_planes(b, 0), 0)[1], 0)
        for zp in range(2):
            ybuf2[k, zp, rows, :] = zsend[k, me, zp]

    def inverse_y(k):
        arrived(zsend.at[k, 0:31], recv.at[3, k])
        o = dot(weights[4], jnp.concatenate([ybuf2[k, 0], ybuf2[k, 1]], axis=1))
        for zp in range(2):
            yout2[k, zp] = o[:, 128 * zp : 128 * (zp + 1)].astype(BF16)
        for d in range(1, NX):
            to = lax.rem(gx + d, NX)
            rows = pl.ds(pl.multiple_of(64 * to, 64), 64)
            remote(yout2.at[k, :, rows, :], pbuf.at[k, gx], 4, k, dev(to, gy, gz))
        rows = pl.ds(pl.multiple_of(64 * gx, 64), 64)
        for zp in range(2):
            pbuf[k, gx, zp] = yout2[k, zp, rows, :]

    def inverse_x(k):
        arrived(pbuf.at[k, 0:7], recv.at[4, k])
        for zp in range(2):
            for t in range(4):
                a, b = exchange_halves(pbuf[k, 2 * t, zp].astype(F32), pbuf[k, 2 * t + 1, zp].astype(F32))
                xg[k, 2 * zp, :, 128 * t : 128 * (t + 1)] = a.astype(BF16)
                xg[k, 2 * zp + 1, :, 128 * t : 128 * (t + 1)] = b.astype(BF16)
        o = dot_t(xg[k].reshape(256, N), weights[5])
        xout[k] = o.astype(BF16).reshape(4, 64, N)
        slab = pl.ds(16 * gy + 4 * k, 4)
        for d in range(1, NY):
            to = lax.rem(gy + d, NY)
            columns = pl.ds(pl.multiple_of(128 * to, 128), 128)
            remote(xout.at[k, :, :, columns], out.at[slab], 5, 0, dev(gx, to, gz))
        columns = pl.ds(pl.multiple_of(128 * gy, 128), 128)
        pltpu.make_async_copy(xout.at[k, :, :, columns], out.at[slab], lsem).start()

    loads[0].wait()
    forward_x(0)
    loads[1].wait()
    forward_x(1)
    forward_y(0)
    forward_x(2)
    forward_y(1)
    forward_x(3)
    forward_y(2)
    forward_y(3)
    for k in range(K):
        to_z_rows(k)
    loads[2].wait()
    along_z()
    for k in range(K):
        from_z_rows(k)
    loads[4].wait()
    loads[5].wait()
    inverse_y(0)
    for k in range(1, K):
        inverse_y(k)
        inverse_x(k - 1)
    inverse_x(K - 1)

    arrived(out.at[0:48], recv.at[5, 0])
    arrived(out.at[0:16], lsem)
    arrived(out.at[0:48], send.at[0])
    arrived(out.at[0:48], send.at[5])
    arrived(psend.at[:, 0:7], send.at[1])
    arrived(psend.at[:, 0:7], send.at[4])
    arrived(zbuf.at[:, 0:31], send.at[2])
    arrived(zbuf.at[:, 0:31], send.at[3])


def on_device(source, *rest):
    pieces = pltpu.VMEM((K, NX, 2, 64, 128), BF16)
    planes = pltpu.VMEM((K, 2, N, 128), BF16)
    lines = pltpu.VMEM((K, NZ * NY, 2, 16, 128), BF16)
    rows = pltpu.VMEM((K, 4, 64, N), BF16)
    return pl.pallas_call(
        kernel,
        out_shape=jax.ShapeDtypeStruct(source.shape, BF16),
        in_specs=[pl.BlockSpec(memory_space=pl.ANY)] * 10,
        out_specs=pl.BlockSpec(memory_space=pl.ANY),
        scratch_shapes=[
            rows,
            pieces,
            planes,
            planes,
            lines,
            pltpu.VMEM((8 * PITCH, 128), F32),
            pltpu.VMEM((N, 1024), F32),
            pltpu.VMEM((N, 1024), BF16),
            pltpu.VMEM((K, 8 * OPITCH, 128), F32),
            lines,
            planes,
            planes,
            pieces,
            rows,
            rows,
            pltpu.VMEM((6, N, N), BF16),
            pltpu.VMEM((N, N), BF16),
            pltpu.SMEM((N,), F32),
            pltpu.SMEM((N,), F32),
            pltpu.SMEM((N,), F32),
            pltpu.SemaphoreType.DMA((6, K)),
            pltpu.SemaphoreType.DMA((6,)),
            pltpu.SemaphoreType.DMA((6,)),
            pltpu.SemaphoreType.DMA((3,)),
            pltpu.SemaphoreType.DMA,
        ],
        compiler_params=pltpu.CompilerParams(
            collective_id=0, has_side_effects=True, vmem_limit_bytes=60 * 1024 * 1024
        ),
    )(source, *rest)


def solution(mesh):
    return jax.shard_map(
        on_device,
        mesh=mesh,
        in_specs=(P("gz", "gx", "gy"),) + (P(),) * 9,
        out_specs=P("gz", "gx", "gy"),
        check_vma=False,
    )
```

```python
import jax
import jax.numpy as jnp
from jax import lax
from jax.experimental import pallas as pl
from jax.experimental.pallas import tpu as pltpu
from jax.sharding import PartitionSpec as P

MESH = pl.DeviceIdType.MESH
F32 = jnp.float32
BF16 = jnp.bfloat16
NX, NY, NZ = 8, 4, 8
N = 512
PAIRS = 8
FORWARD = ((0, 1), (1, 1), (2, 2), (4, 2), (6, 2))
INVERSE = ((0, 1), (1, 2), (3, 2), (5, 1), (6, 1), (7, 1))
FORWARD_ORDER = (
    ("x", 0), ("x", 1), ("x", 2), ("y", 0), ("z", 0, 0), ("z", 0, 1), ("y", 1), ("z", 1, 0), ("z", 1, 1),
    ("x", 3), ("y", 2), ("z", 2, 0), ("z", 2, 1), ("x", 4), ("y", 3), ("z", 3, 0), ("y", 4), ("z", 4, 0),
    ("z", 3, 1), ("z", 4, 1),
)
INVERSE_ORDER = (("y", 0), ("y", 1), ("x", 0), ("y", 2), ("x", 1), ("y", 3), ("x", 2), ("y", 4), ("x", 3), ("y", 5), ("x", 4), ("x", 5))
PITCH = N + 8
FAR_FIRST = (4, 3, 5, 2, 6, 1, 7)


def dot(a, b):
    return jnp.dot(a, b, preferred_element_type=F32)


def dot_t(a, b):
    return lax.dot_general(a, b, (((1,), (1,)), ((), ())), preferred_element_type=F32)


def kernel(
    src, fx, fy, fz, ix, iy, iz, vx, vy, vz, out,
    staged, xin, psend, ybuf, yout, zbuf, zlines, recip, scaled, olines, zsend, ybuf2, yout2, pbuf, xg, xout,
    weights, izp, vxs, vys, vzs, recv, send, wsem, vsem, ssem,
):
    gx, gy, gz = lax.axis_index("gx"), lax.axis_index("gy"), lax.axis_index("gz")
    x_hi, x_lo, core = lax.rem(gx, 2), gy // 2, lax.rem(gy, 2)

    def xor(a, b):
        return a + b - 2 * a * b

    def slab_of(b):
        return 2 * xor(b // 2, x_hi) + lax.rem(b, 2)

    def same_slab(a):
        return 2 * xor(slab // 2, lax.rem(a, 2)) + core

    slab = slab_of(gy)
    me = gz * NY + slab

    def dev(a, b, c):
        return {"gx": a, "gy": b, "gz": c}

    def plane_peer(d):
        to = lax.rem(gx + d, NX)
        return dev(to, same_slab(to), gz)

    def remote(s, d, stage, k, where):
        pltpu.make_async_remote_copy(
            src_ref=s, dst_ref=d, send_sem=send.at[stage], recv_sem=recv.at[stage, k],
            device_id=where, device_id_type=MESH,
        ).start()

    def arrived(ref, sem, name="end"):
        with jax.named_scope(f"w_{name}"):
            pltpu.make_async_copy(ref, ref, sem).wait()

    barrier = pltpu.get_barrier_semaphore()
    for d in range(1, NX):
        pl.semaphore_signal(barrier, inc=1, device_id=plane_peer(d), device_id_type=MESH)
    for c in range(NZ):
        for b in range(NY):
            if b or c:
                pl.semaphore_signal(
                    barrier, inc=1, device_id=dev(gx, lax.rem(gy + b, NY), lax.rem(gz + c, NZ)), device_id_type=MESH
                )

    stage_in = pltpu.make_async_copy(src, staged, ssem)
    stage_in.start()
    my_columns = pl.ds(pl.multiple_of(128 * gy, 128), 128)
    for k, (p, n) in enumerate(FORWARD):
        for j in range(p, p + n):
            pltpu.make_async_copy(
                src.at[pl.ds(16 * slab + 2 * j, 2)], xin.at[j, :, :, my_columns], recv.at[0, k]
            ).start()
    loads = [pltpu.make_async_copy(w, weights.at[i], wsem.at[i]) for i, w in enumerate((fx, fy, fz, iz, iy, ix))]
    for c in loads:
        c.start()
    vloads = [pltpu.make_async_copy(v, s, vsem.at[i]) for i, (v, s) in enumerate(((vx, vxs), (vy, vys), (vz, vzs)))]
    for c in vloads:
        c.start()

    with jax.named_scope("w_barrier"):
        pl.semaphore_wait(barrier, NX - 1 + NZ * NY - 1)
    stage_in.wait()

    for k, (p, n) in enumerate(FORWARD):
        for to in (2 * (1 - x_lo), 2 * (1 - x_lo) + 1, 2 * x_lo + 1 - core):
            for j in range(p, p + n):
                remote(
                    staged.at[pl.ds(16 * slab_of(to) + 2 * j, 2)],
                    xin.at[j, :, :, my_columns],
                    0, k, dev(gx, to, gz),
                )

    lane = lax.broadcasted_iota(jnp.int32, (8, 128), 1)
    sub = lax.broadcasted_iota(jnp.int32, (8, 128), 0)
    low = lane < 64

    def exchange_halves(a, b):
        keep = jnp.broadcast_to(lax.broadcasted_iota(jnp.int32, (1, 128), 1) < 64, a.shape)
        return (
            jnp.where(keep, a, pltpu.roll(b, 64, 1)),
            jnp.where(keep, pltpu.roll(a, 64, 1), b),
        )

    for c in vloads:
        c.wait()
    along_p = jnp.zeros((8, 128), F32)
    for i in range(64):
        along_p = jnp.where((lane & 63) == i, vxs[64 * gx + i], along_p)
    along_qp = [
        along_p + jnp.where(low, vys[16 * me + q], vys[16 * me + q + 8]) for q in range(8)
    ]

    def reciprocals(g, _):
        col = jnp.zeros((8, 128), F32)
        for i in range(8):
            col = jnp.where(sub == i, vzs[8 * g + i], col)
        rows = pl.ds(pl.multiple_of(8 * g, 8), 8)
        for q in range(8):
            recip[rows, 128 * q : 128 * (q + 1)] = 1.0 / (col + along_qp[q])
        return 0

    lax.fori_loop(0, N // 8, reciprocals, 0)

    loads[3].wait()
    row = lax.broadcasted_iota(jnp.int32, (N, N), 0)
    wanted = ((row & 63) >> 1) * 16 + (row >> 6) * 2 + (row & 1)
    order = (lax.broadcasted_iota(jnp.int32, (N, N), 1) == wanted).astype(F32).astype(BF16)
    izp[...] = dot(order, weights[3]).astype(BF16)

    my_block = pl.ds(pl.multiple_of(64 * gx, 64), 64)
    my_lines = pl.ds(pl.multiple_of(16 * me, 16), 16)

    def forward_x(k):
        p, n = FORWARD[k]
        arrived(xin.at[p : p + n], recv.at[0, k], f"x{k}")
        o = dot_t(xin[p : p + n].reshape(128 * n, N), weights[0]).reshape(n, 2, 64, N)
        for j in range(n):
            for t in range(4):
                a, b = exchange_halves(o[j, 0, :, 128 * t : 128 * (t + 1)], o[j, 1, :, 128 * t : 128 * (t + 1)])
                psend[2 * t, p + j] = a.astype(BF16)
                psend[2 * t + 1, p + j] = b.astype(BF16)
        for d in range(1, NX):
            to = lax.rem(gx + d, NX)
            remote(psend.at[to, p : p + n], ybuf.at[p : p + n, my_block, :], 1, k, plane_peer(d))
        for j in range(p, p + n):
            ybuf[j, my_block, :] = psend[gx, j]

    to_gz = [lax.rem(gz + c, NZ) for c in range(NZ)]
    near = [[2 * x_lo + c, 2 * (1 - x_lo) + c] for c in range(2)]
    near_slab = [[slab_of(b) for b in pair] for pair in near]
    partner = 2 * x_lo + 1 - core

    def line_peers(half):
        for c in FAR_FIRST:
            for b, place in zip(near[half], near_slab[half]):
                yield to_gz[c] * NY + place, dev(gx, b, to_gz[c])
        yield gz * NY + near_slab[half][1], dev(gx, near[half][1], gz)
        if half == 0:
            yield gz * NY + slab_of(partner), dev(gx, partner, gz)

    def forward_y(k):
        p, n = FORWARD[k]
        arrived(psend.at[0 : NX - 1, p : p + n], recv.at[1, k], f"y{k}")
        o = dot(weights[1], jnp.concatenate([ybuf[j] for j in range(p, p + n)], axis=1))
        for j in range(n):
            yout[p + j] = o[:, 128 * j : 128 * (j + 1)].astype(BF16)

        for j in range(p, p + n):
            zbuf[me, j] = yout[j, my_lines, :]

    def send_lines(k, half):
        p, n = FORWARD[k]
        for place, where in line_peers(half):
            rows = pl.ds(pl.multiple_of(16 * place, 16), 16)
            remote(yout.at[p : p + n, rows, :], zbuf.at[me, p : p + n], 2, k, where)

    def to_z_rows(k):
        p, n = FORWARD[k]
        arrived(zbuf.at[0 : NZ * NY - 1, p : p + n], recv.at[2, k], f"z{k}")

        def some(g, _):
            for s in range(8):
                for j in range(p, p + n):
                    tile = zbuf[8 * g + s, j].astype(F32)
                    a, b = exchange_halves(tile[:8], tile[8:])
                    z = 16 * (8 * g + s) + 2 * j
                    zlines[pl.ds(z, 8, stride=PITCH), :] = a
                    zlines[pl.ds(z + 1, 8, stride=PITCH), :] = b
            return 0

        lax.fori_loop(0, 4, some, 0)

    def along_z():
        for h in range(4):
            d = jnp.concatenate(
                [zlines[PITCH * q : PITCH * q + N, :] for q in (2 * h, 2 * h + 1)], axis=1
            ).astype(BF16)
            c = dot(weights[2], d).astype(BF16).astype(F32)
            scaled[:, 256 * h : 256 * (h + 1)] = (c * recip[:, 256 * h : 256 * (h + 1)]).astype(BF16)

    def from_z_rows(k):
        p, n = INVERSE[k]
        for h in range(4):
            o = dot(izp[64 * p : 64 * (p + n), :], scaled[:, 256 * h : 256 * (h + 1)])
            for j in range(2):
                at = PITCH * (2 * h + j) + 64 * p
                olines[at : at + 64 * n, :] = o[:, 128 * j : 128 * (j + 1)]

        def some(g, _):
            for s in range(8):
                for j in range(p, p + n):
                    at = 64 * j + 2 * (8 * g + s)
                    a, b = exchange_halves(
                        olines[pl.ds(at, 8, stride=PITCH), :], olines[pl.ds(at + 1, 8, stride=PITCH), :]
                    )
                    zsend[8 * g + s, j] = jnp.concatenate([a, b], axis=0).astype(BF16)
            return 0

        lax.fori_loop(0, 4, some, 0)

        for half in range(2):
            for place, where in line_peers(half):
                remote(zsend.at[place, p : p + n], ybuf2.at[p : p + n, my_lines, :], 3, k, where)
        for j in range(p, p + n):
            ybuf2[j, my_lines, :] = zsend[me, j]

    def inverse_y(k):
        p, n = INVERSE[k]
        arrived(zsend.at[0 : NZ * NY - 1, p : p + n], recv.at[3, k], f"yi{k}")
        o = dot(weights[4], jnp.concatenate([ybuf2[j] for j in range(p, p + n)], axis=1))
        for j in range(n):
            yout2[p + j] = o[:, 128 * j : 128 * (j + 1)].astype(BF16)
        for d in range(1, NX):
            to = lax.rem(gx + d, NX)
            rows = pl.ds(pl.multiple_of(64 * to, 64), 64)
            remote(yout2.at[p : p + n, rows, :], pbuf.at[gx, p : p + n], 4, k, plane_peer(d))
        for j in range(p, p + n):
            pbuf[gx, j] = yout2[j, my_block, :]

    def inverse_x(k):
        p, n = INVERSE[k]
        arrived(pbuf.at[0 : NX - 1, p : p + n], recv.at[4, k], f"xi{k}")
        for j in range(p, p + n):
            for t in range(4):
                a, b = exchange_halves(pbuf[2 * t, j].astype(F32), pbuf[2 * t + 1, j].astype(F32))
                xg[2 * j, :, 128 * t : 128 * (t + 1)] = a.astype(BF16)
                xg[2 * j + 1, :, 128 * t : 128 * (t + 1)] = b.astype(BF16)
        here = slice(2 * p, 2 * (p + n))
        o = dot_t(xg[here].reshape(128 * n, N), weights[5])
        xout[here] = o.astype(BF16).reshape(2 * n, 64, N)
        mine = pl.ds(16 * slab + 2 * p, 2 * n)
        for d in (2, 3, 1):
            to = lax.rem(gy + d, NY)
            columns = pl.ds(pl.multiple_of(128 * to, 128), 128)
            remote(xout.at[here, :, columns], out.at[mine], 5, 0, dev(gx, to, gz))
        out[mine] = xout[here, :, my_columns]

    loads[0].wait()
    loads[1].wait()
    for stage, *k in FORWARD_ORDER:
        {"x": forward_x, "y": forward_y, "z": send_lines}[stage](*k)
    for k in range(len(FORWARD)):
        to_z_rows(k)
    loads[2].wait()
    with jax.named_scope("c_z"):
        along_z()
    for k in range(len(INVERSE)):
        with jax.named_scope(f"c_from{k}"):
            from_z_rows(k)
    loads[4].wait()
    loads[5].wait()
    for stage, k in INVERSE_ORDER:
        (inverse_x if stage == "x" else inverse_y)(k)

    arrived(staged.at[0:48], recv.at[5, 0])
    arrived(staged.at[0:48], send.at[0])
    arrived(staged.at[0:48], send.at[5])
    arrived(psend.at[0 : NX - 1], send.at[1])
    arrived(psend.at[0 : NX - 1], send.at[4])
    arrived(zbuf.at[0 : NZ * NY - 1], send.at[2])
    arrived(zbuf.at[0 : NZ * NY - 1], send.at[3])


def on_device(source, *rest):
    pieces = pltpu.VMEM((NX, PAIRS, 64, 128), BF16)
    planes = pltpu.VMEM((PAIRS, N, 128), BF16)
    lines = pltpu.VMEM((NZ * NY, PAIRS, 16, 128), BF16)
    pencils = pltpu.VMEM((2 * PAIRS, 64, N), BF16)
    stages = max(len(FORWARD), len(INVERSE))
    return pl.pallas_call(
        kernel,
        out_shape=pltpu.VMEM(source.shape, BF16),
        in_specs=[pl.BlockSpec(memory_space=pl.ANY)] * 10,
        out_specs=pl.BlockSpec(memory_space=pltpu.VMEM),
        scratch_shapes=[
            pltpu.VMEM(source.shape, BF16),
            pltpu.VMEM((PAIRS, 2, 64, N), BF16),
            pieces,
            planes,
            planes,
            lines,
            pltpu.VMEM((8 * PITCH, 128), F32),
            pltpu.VMEM((N, 1024), F32),
            pltpu.VMEM((N, 1024), BF16),
            pltpu.VMEM((8 * PITCH, 128), F32),
            lines,
            planes,
            planes,
            pieces,
            pencils,
            pencils,
            pltpu.VMEM((6, N, N), BF16),
            pltpu.VMEM((N, N), BF16),
            pltpu.SMEM((N,), F32),
            pltpu.SMEM((N,), F32),
            pltpu.SMEM((N,), F32),
            pltpu.SemaphoreType.DMA((6, stages)),
            pltpu.SemaphoreType.DMA((6,)),
            pltpu.SemaphoreType.DMA((6,)),
            pltpu.SemaphoreType.DMA((3,)),
            pltpu.SemaphoreType.DMA,
        ],
        compiler_params=pltpu.CompilerParams(
            collective_id=0, has_side_effects=True, vmem_limit_bytes=60 * 1024 * 1024
        ),
    )(source, *rest)


def solution(mesh):
    return jax.shard_map(
        on_device,
        mesh=mesh,
        in_specs=(P("gz", "gx", "gy"),) + (P(),) * 9,
        out_specs=P("gz", "gx", "gy"),
        check_vma=False,
    )
```

```python
import jax
import jax.numpy as jnp
from jax import lax
from jax.experimental import pallas as pl
from jax.experimental.pallas import tpu as pltpu
from jax.sharding import PartitionSpec as P

MESH = pl.DeviceIdType.MESH
F32 = jnp.float32
BF16 = jnp.bfloat16
NX, NY, NZ = 8, 4, 8
N = 512
PAIRS = 8
FORWARD = ((0, 1), (1, 1), (2, 2), (4, 2), (6, 2))
INVERSE = ((0, 1), (1, 2), (3, 2), (5, 1), (6, 1), (7, 1))
FORWARD_ORDER = (
    ("x", 0), ("x", 1), ("x", 2), ("y", 0), ("z", 0, 0), ("z", 0, 1), ("y", 1), ("z", 1, 0), ("z", 1, 1),
    ("x", 3), ("y", 2), ("z", 2, 0), ("z", 2, 1), ("x", 4), ("y", 3), ("z", 3, 0), ("y", 4), ("z", 4, 0),
    ("z", 3, 1), ("z", 4, 1),
)
INVERSE_ORDER = (
    ("y", 0), ("y", 1), ("x", 0), ("y", 2), ("x", 1), ("y", 3), ("y", 4), ("x", 2), ("y", 5), ("x", 3), ("x", 4), ("x", 5),
)
PITCH = N + 8
FAR_FIRST = (4, 3, 5, 2, 6, 1, 7)
PLANE_FAR_FIRST = ((2, 1), (1, 1), (3, 1), (2, 0), (0, 1), (1, 0), (3, 0))


def dot(a, b):
    return jnp.dot(a, b, preferred_element_type=F32)


def dot_t(a, b):
    return lax.dot_general(a, b, (((1,), (1,)), ((), ())), preferred_element_type=F32)


def kernel(
    src, fx, fy, fz, ix, iy, iz, vx, vy, vz, out,
    staged, xin, psend, ybuf, yout, zbuf, zlines, recip, scaled, olines, zsend, ybuf2, yout2, pbuf, xg, xout,
    weights, izp, vxs, vys, vzs, recv, send, wsem, vsem, ssem, ready,
):
    gx, gy, gz = lax.axis_index("gx"), lax.axis_index("gy"), lax.axis_index("gz")
    x_hi, x_lo, core = lax.rem(gx, 2), gy // 2, lax.rem(gy, 2)

    def xor(a, b):
        return a + b - 2 * a * b

    def slab_of(b):
        return 2 * xor(b // 2, x_hi) + lax.rem(b, 2)

    def same_slab(a):
        return 2 * xor(slab // 2, lax.rem(a, 2)) + core

    slab = slab_of(gy)
    me = gz * NY + slab

    def dev(a, b, c):
        return {"gx": a, "gy": b, "gz": c}

    plane_peers = []
    for d, h in PLANE_FAR_FIRST:
        to = 2 * lax.rem(gx // 2 + d, NX // 2) + (xor(x_hi, 1) if h else x_hi)
        plane_peers.append((to, dev(to, same_slab(to), gz)))

    def remote(s, d, stage, k, where):
        pltpu.make_async_remote_copy(
            src_ref=s, dst_ref=d, send_sem=send.at[stage], recv_sem=recv.at[stage, k],
            device_id=where, device_id_type=MESH,
        ).start()

    def arrived(ref, sem, name="end"):
        with jax.named_scope(f"w_{name}"):
            pltpu.make_async_copy(ref, ref, sem).wait()

    barrier = pltpu.get_barrier_semaphore()
    for _, where in plane_peers:
        pl.semaphore_signal(barrier, inc=1, device_id=where, device_id_type=MESH)
    for b in range(1, NY):
        pl.semaphore_signal(barrier, inc=1, device_id=dev(gx, lax.rem(gy + b, NY), gz), device_id_type=MESH)
    for c in range(1, NZ):
        @pl.when(c > gz)
        def _():
            for b in range(NY):
                pl.semaphore_signal(barrier, inc=1, device_id=dev(gx, b, c), device_id_type=MESH)

    stage_in = pltpu.make_async_copy(src, staged, ssem)
    stage_in.start()
    my_columns = pl.ds(pl.multiple_of(128 * gy, 128), 128)
    for k, (p, n) in enumerate(FORWARD):
        for j in range(p, p + n):
            pltpu.make_async_copy(
                src.at[pl.ds(16 * slab + 2 * j, 2)], xin.at[j, :, :, my_columns], recv.at[0, k]
            ).start()
    loads = [pltpu.make_async_copy(w, weights.at[i], wsem.at[i]) for i, w in enumerate((fx, fy, fz, iz, iy, ix))]
    for c in loads:
        c.start()
    vloads = [pltpu.make_async_copy(v, s, vsem.at[i]) for i, (v, s) in enumerate(((vx, vxs), (vy, vys), (vz, vzs)))]
    for c in vloads:
        c.start()

    with jax.named_scope("w_barrier"):
        pl.semaphore_wait(barrier, NX - 1 + NY - 1 + NY * gz)
    stage_in.wait()

    for k, (p, n) in enumerate(FORWARD):
        for to in (2 * (1 - x_lo), 2 * (1 - x_lo) + 1, 2 * x_lo + 1 - core):
            for j in range(p, p + n):
                remote(
                    staged.at[pl.ds(16 * slab_of(to) + 2 * j, 2)],
                    xin.at[j, :, :, my_columns],
                    0, k, dev(gx, to, gz),
                )

    for c in range(NZ - 1):
        @pl.when(c < gz)
        def _():
            for b in range(NY):
                pl.semaphore_signal(ready, inc=1, device_id=dev(gx, b, c), device_id_type=MESH)

    lane = lax.broadcasted_iota(jnp.int32, (8, 128), 1)
    sub = lax.broadcasted_iota(jnp.int32, (8, 128), 0)
    low = lane < 64

    def exchange_halves(a, b):
        keep = jnp.broadcast_to(lax.broadcasted_iota(jnp.int32, (1, 128), 1) < 64, a.shape)
        return (
            jnp.where(keep, a, pltpu.roll(b, 64, 1)),
            jnp.where(keep, pltpu.roll(a, 64, 1), b),
        )

    for c in vloads:
        c.wait()
    along_p = jnp.zeros((8, 128), F32)
    for i in range(64):
        along_p = jnp.where((lane & 63) == i, vxs[64 * gx + i], along_p)
    along_qp = [
        along_p + jnp.where(low, vys[16 * me + q], vys[16 * me + q + 8]) for q in range(8)
    ]

    def reciprocals(g, _):
        col = jnp.zeros((8, 128), F32)
        for i in range(8):
            col = jnp.where(sub == i, vzs[8 * g + i], col)
        rows = pl.ds(pl.multiple_of(8 * g, 8), 8)
        for q in range(8):
            recip[rows, 128 * q : 128 * (q + 1)] = 1.0 / (col + along_qp[q])
        return 0

    lax.fori_loop(0, N // 8, reciprocals, 0)

    loads[3].wait()
    row = lax.broadcasted_iota(jnp.int32, (N, N), 0)
    wanted = ((row & 63) >> 1) * 16 + (row >> 6) * 2 + (row & 1)
    order = (lax.broadcasted_iota(jnp.int32, (N, N), 1) == wanted).astype(F32).astype(BF16)
    izp[...] = dot(order, weights[3]).astype(BF16)

    my_block = pl.ds(pl.multiple_of(64 * gx, 64), 64)
    my_lines = pl.ds(pl.multiple_of(16 * me, 16), 16)

    def forward_x(k):
        p, n = FORWARD[k]
        arrived(xin.at[p : p + n], recv.at[0, k], f"x{k}")
        o = dot_t(xin[p : p + n].reshape(128 * n, N), weights[0]).reshape(n, 2, 64, N)
        for j in range(n):
            for t in range(4):
                a, b = exchange_halves(o[j, 0, :, 128 * t : 128 * (t + 1)], o[j, 1, :, 128 * t : 128 * (t + 1)])
                psend[2 * t, p + j] = a.astype(BF16)
                psend[2 * t + 1, p + j] = b.astype(BF16)
        for to, where in plane_peers:
            remote(psend.at[to, p : p + n], ybuf.at[p : p + n, my_block, :], 1, k, where)
        for j in range(p, p + n):
            ybuf[j, my_block, :] = psend[gx, j]

    to_gz = [lax.rem(gz + c, NZ) for c in range(NZ)]
    near = [[2 * x_lo + c, 2 * (1 - x_lo) + c] for c in range(2)]
    near_slab = [[slab_of(b) for b in pair] for pair in near]
    partner = 2 * x_lo + 1 - core

    def line_peers(half):
        for c in FAR_FIRST:
            for b, place in zip(near[half], near_slab[half]):
                yield to_gz[c] * NY + place, dev(gx, b, to_gz[c])
        yield gz * NY + near_slab[half][1], dev(gx, near[half][1], gz)
        if half == 0:
            yield gz * NY + slab_of(partner), dev(gx, partner, gz)

    def forward_y(k):
        p, n = FORWARD[k]
        arrived(psend.at[0 : NX - 1, p : p + n], recv.at[1, k], f"y{k}")
        o = dot(weights[1], jnp.concatenate([ybuf[j] for j in range(p, p + n)], axis=1))
        for j in range(n):
            yout[p + j] = o[:, 128 * j : 128 * (j + 1)].astype(BF16)

        for j in range(p, p + n):
            zbuf[me, j] = yout[j, my_lines, :]

    def send_lines(k, half):
        p, n = FORWARD[k]
        if (k, half) == (0, 0):
            @pl.when(gz < NZ - 1)
            def _():
                pl.semaphore_wait(ready, NY * (NZ - 1 - gz))

        for place, where in line_peers(half):
            rows = pl.ds(pl.multiple_of(16 * place, 16), 16)
            remote(yout.at[p : p + n, rows, :], zbuf.at[me, p : p + n], 2, k, where)

    def to_z_rows(k):
        p, n = FORWARD[k]
        arrived(zbuf.at[0 : NZ * NY - 1, p : p + n], recv.at[2, k], f"z{k}")

        def some(g, _):
            for s in range(8):
                for j in range(p, p + n):
                    tile = zbuf[8 * g + s, j].astype(F32)
                    a, b = exchange_halves(tile[:8], tile[8:])
                    z = 16 * (8 * g + s) + 2 * j
                    zlines[pl.ds(z, 8, stride=PITCH), :] = a
                    zlines[pl.ds(z + 1, 8, stride=PITCH), :] = b
            return 0

        lax.fori_loop(0, 4, some, 0)

    def along_z():
        for h in range(4):
            d = jnp.concatenate(
                [zlines[PITCH * q : PITCH * q + N, :] for q in (2 * h, 2 * h + 1)], axis=1
            ).astype(BF16)
            c = dot(weights[2], d).astype(BF16).astype(F32)
            scaled[:, 256 * h : 256 * (h + 1)] = (c * recip[:, 256 * h : 256 * (h + 1)]).astype(BF16)

    def from_z_rows(k):
        p, n = INVERSE[k]
        for h in range(4):
            o = dot(izp[64 * p : 64 * (p + n), :], scaled[:, 256 * h : 256 * (h + 1)])
            for j in range(2):
                at = PITCH * (2 * h + j) + 64 * p
                olines[at : at + 64 * n, :] = o[:, 128 * j : 128 * (j + 1)]

        def some(g, _):
            for s in range(8):
                for j in range(p, p + n):
                    at = 64 * j + 2 * (8 * g + s)
                    a, b = exchange_halves(
                        olines[pl.ds(at, 8, stride=PITCH), :], olines[pl.ds(at + 1, 8, stride=PITCH), :]
                    )
                    zsend[8 * g + s, j] = jnp.concatenate([a, b], axis=0).astype(BF16)
            return 0

        lax.fori_loop(0, 4, some, 0)

        for half in range(2):
            for place, where in line_peers(half):
                remote(zsend.at[place, p : p + n], ybuf2.at[p : p + n, my_lines, :], 3, k, where)
        for j in range(p, p + n):
            ybuf2[j, my_lines, :] = zsend[me, j]

    def inverse_y(k):
        p, n = INVERSE[k]
        arrived(zsend.at[0 : NZ * NY - 1, p : p + n], recv.at[3, k], f"yi{k}")
        o = dot(weights[4], jnp.concatenate([ybuf2[j] for j in range(p, p + n)], axis=1))
        for j in range(n):
            yout2[p + j] = o[:, 128 * j : 128 * (j + 1)].astype(BF16)
        for to, where in plane_peers:
            rows = pl.ds(pl.multiple_of(64 * to, 64), 64)
            remote(yout2.at[p : p + n, rows, :], pbuf.at[gx, p : p + n], 4, k, where)
        for j in range(p, p + n):
            pbuf[gx, j] = yout2[j, my_block, :]

    def inverse_x(k):
        p, n = INVERSE[k]
        arrived(pbuf.at[0 : NX - 1, p : p + n], recv.at[4, k], f"xi{k}")
        for j in range(p, p + n):
            for t in range(4):
                a, b = exchange_halves(pbuf[2 * t, j].astype(F32), pbuf[2 * t + 1, j].astype(F32))
                xg[2 * j, :, 128 * t : 128 * (t + 1)] = a.astype(BF16)
                xg[2 * j + 1, :, 128 * t : 128 * (t + 1)] = b.astype(BF16)
        here = slice(2 * p, 2 * (p + n))
        o = dot_t(xg[here].reshape(128 * n, N), weights[5])
        xout[here] = o.astype(BF16).reshape(2 * n, 64, N)
        mine = pl.ds(16 * slab + 2 * p, 2 * n)
        for d in (2, 3, 1):
            to = lax.rem(gy + d, NY)
            columns = pl.ds(pl.multiple_of(128 * to, 128), 128)
            remote(xout.at[here, :, columns], out.at[mine], 5, 0, dev(gx, to, gz))
        out[mine] = xout[here, :, my_columns]

    loads[0].wait()
    loads[1].wait()
    for stage, *k in FORWARD_ORDER:
        {"x": forward_x, "y": forward_y, "z": send_lines}[stage](*k)
    for k in range(len(FORWARD)):
        to_z_rows(k)
    loads[2].wait()
    with jax.named_scope("c_z"):
        along_z()
    for k in range(len(INVERSE)):
        with jax.named_scope(f"c_from{k}"):
            from_z_rows(k)
    loads[4].wait()
    loads[5].wait()
    for stage, k in INVERSE_ORDER:
        (inverse_x if stage == "x" else inverse_y)(k)

    arrived(staged.at[0:48], recv.at[5, 0])
    arrived(staged.at[0:48], send.at[0])
    arrived(staged.at[0:48], send.at[5])
    arrived(psend.at[0 : NX - 1], send.at[1])
    arrived(psend.at[0 : NX - 1], send.at[4])
    arrived(zbuf.at[0 : NZ * NY - 1], send.at[2])
    arrived(zbuf.at[0 : NZ * NY - 1], send.at[3])


def on_device(source, *rest):
    pieces = pltpu.VMEM((NX, PAIRS, 64, 128), BF16)
    planes = pltpu.VMEM((PAIRS, N, 128), BF16)
    lines = pltpu.VMEM((NZ * NY, PAIRS, 16, 128), BF16)
    pencils = pltpu.VMEM((2 * PAIRS, 64, N), BF16)
    stages = max(len(FORWARD), len(INVERSE))
    return pl.pallas_call(
        kernel,
        out_shape=pltpu.VMEM(source.shape, BF16),
        in_specs=[pl.BlockSpec(memory_space=pl.ANY)] * 10,
        out_specs=pl.BlockSpec(memory_space=pltpu.VMEM),
        scratch_shapes=[
            pltpu.VMEM(source.shape, BF16),
            pltpu.VMEM((PAIRS, 2, 64, N), BF16),
            pieces,
            planes,
            planes,
            lines,
            pltpu.VMEM((8 * PITCH, 128), F32),
            pltpu.VMEM((N, 1024), F32),
            pltpu.VMEM((N, 1024), BF16),
            pltpu.VMEM((8 * PITCH, 128), F32),
            lines,
            planes,
            planes,
            pieces,
            pencils,
            pencils,
            pltpu.VMEM((6, N, N), BF16),
            pltpu.VMEM((N, N), BF16),
            pltpu.SMEM((N,), F32),
            pltpu.SMEM((N,), F32),
            pltpu.SMEM((N,), F32),
            pltpu.SemaphoreType.DMA((6, stages)),
            pltpu.SemaphoreType.DMA((6,)),
            pltpu.SemaphoreType.DMA((6,)),
            pltpu.SemaphoreType.DMA((3,)),
            pltpu.SemaphoreType.DMA,
            pltpu.SemaphoreType.REGULAR,
        ],
        compiler_params=pltpu.CompilerParams(
            collective_id=0, has_side_effects=True, vmem_limit_bytes=60 * 1024 * 1024
        ),
    )(source, *rest)


def solution(mesh):
    return jax.shard_map(
        on_device,
        mesh=mesh,
        in_specs=(P("gz", "gx", "gy"),) + (P(),) * 9,
        out_specs=P("gz", "gx", "gy"),
        check_vma=False,
    )
```

```python
import jax
import jax.numpy as jnp
from jax import lax
from jax.experimental import pallas as pl
from jax.experimental.pallas import tpu as pltpu
from jax.sharding import PartitionSpec as P

MESH = pl.DeviceIdType.MESH
F32 = jnp.float32
BF16 = jnp.bfloat16
NX, NY, NZ = 8, 4, 8
N = 512
EARLY = 2
PAIRS = 8
FORWARD = ((0, 1), (1, 1), (2, 2), (4, 2), (6, 2))
INVERSE = ((0, 1), (1, 2), (3, 2), (5, 1), (6, 1), (7, 1))
FORWARD_ORDER = (
    ("x", 0), ("x", 1), ("x", 2), ("y", 0), ("z", 0, 0), ("z", 0, 1), ("y", 1), ("z", 1, 0), ("z", 1, 1),
    ("x", 3), ("y", 2), ("z", 2, 0), ("z", 2, 1), ("x", 4), ("y", 3), ("z", 3, 0), ("y", 4), ("z", 4, 0),
    ("z", 3, 1), ("z", 4, 1),
)
INVERSE_ORDER = (
    ("y", 0), ("y", 1), ("x", 0), ("y", 2), ("x", 1), ("y", 3), ("y", 4), ("x", 2), ("y", 5), ("x", 3), ("x", 4), ("x", 5),
)
PITCH = N + 8
FAR_FIRST = (4, 3, 5, 2, 6, 1, 7)
PLANE_FAR_FIRST = ((2, 1), (1, 1), (3, 1), (2, 0), (0, 1), (1, 0), (3, 0))


def dot(a, b):
    return jnp.dot(a, b, preferred_element_type=F32)


def dot_t(a, b):
    return lax.dot_general(a, b, (((1,), (1,)), ((), ())), preferred_element_type=F32)


def kernel(
    src, fx, fy, fz, ix, iy, iz, vx, vy, vz, out,
    staged, xin, psend, ybuf, yout, zbuf, zlines, recip, scaled, olines, zsend, ybuf2, yout2, pbuf, xg, xout,
    weights, izp, vxs, vys, vzs, recv, send, wsem, vsem, ssem, ready,
):
    gx, gy, gz = lax.axis_index("gx"), lax.axis_index("gy"), lax.axis_index("gz")
    x_hi, x_lo, core = lax.rem(gx, 2), gy // 2, lax.rem(gy, 2)

    def xor(a, b):
        return a + b - 2 * a * b

    def slab_of(b):
        return 2 * xor(b // 2, x_hi) + lax.rem(b, 2)

    def same_slab(a):
        return 2 * xor(slab // 2, lax.rem(a, 2)) + core

    slab = slab_of(gy)
    me = gz * NY + slab

    def dev(a, b, c):
        return {"gx": a, "gy": b, "gz": c}

    plane_peers = []
    for d, h in PLANE_FAR_FIRST:
        to = 2 * lax.rem(gx // 2 + d, NX // 2) + (xor(x_hi, 1) if h else x_hi)
        plane_peers.append((to, dev(to, same_slab(to), gz)))

    def remote(s, d, stage, k, where):
        pltpu.make_async_remote_copy(
            src_ref=s, dst_ref=d, send_sem=send.at[stage], recv_sem=recv.at[stage, k],
            device_id=where, device_id_type=MESH,
        ).start()

    def arrived(ref, sem, name="end"):
        with jax.named_scope(f"w_{name}"):
            pltpu.make_async_copy(ref, ref, sem).wait()

    barrier = pltpu.get_barrier_semaphore()
    for _, where in plane_peers:
        pl.semaphore_signal(barrier, inc=1, device_id=where, device_id_type=MESH)
    for b in range(1, NY):
        pl.semaphore_signal(barrier, inc=1, device_id=dev(gx, lax.rem(gy + b, NY), gz), device_id_type=MESH)
    for c in range(1, NZ):
        @pl.when((gz < c) & (gz < EARLY))
        def _():
            for b in range(NY):
                pl.semaphore_signal(barrier, inc=1, device_id=dev(gx, b, c), device_id_type=MESH)

    stage_in = pltpu.make_async_copy(src, staged, ssem)
    stage_in.start()
    my_columns = pl.ds(pl.multiple_of(128 * gy, 128), 128)
    for k, (p, n) in enumerate(FORWARD):
        for j in range(p, p + n):
            pltpu.make_async_copy(
                src.at[pl.ds(16 * slab + 2 * j, 2)], xin.at[j, :, :, my_columns], recv.at[0, k]
            ).start()
    loads = [pltpu.make_async_copy(w, weights.at[i], wsem.at[i]) for i, w in enumerate((fx, fy, fz, iz, iy, ix))]
    for c in loads:
        c.start()
    vloads = [pltpu.make_async_copy(v, s, vsem.at[i]) for i, (v, s) in enumerate(((vx, vxs), (vy, vys), (vz, vzs)))]
    for c in vloads:
        c.start()

    with jax.named_scope("w_barrier"):
        pl.semaphore_wait(barrier, NX - 1 + NY - 1 + NY * jnp.minimum(gz, EARLY))
    stage_in.wait()

    for k, (p, n) in enumerate(FORWARD):
        for to in (2 * (1 - x_lo), 2 * (1 - x_lo) + 1, 2 * x_lo + 1 - core):
            for j in range(p, p + n):
                remote(
                    staged.at[pl.ds(16 * slab_of(to) + 2 * j, 2)],
                    xin.at[j, :, :, my_columns],
                    0, k, dev(gx, to, gz),
                )

    for c in range(EARLY):
        @pl.when(c < gz)
        def _():
            for b in range(NY):
                pl.semaphore_signal(ready, inc=1, device_id=dev(gx, b, c), device_id_type=MESH)

    lane = lax.broadcasted_iota(jnp.int32, (8, 128), 1)
    sub = lax.broadcasted_iota(jnp.int32, (8, 128), 0)
    low = lane < 64

    def exchange_halves(a, b):
        keep = jnp.broadcast_to(lax.broadcasted_iota(jnp.int32, (1, 128), 1) < 64, a.shape)
        return (
            jnp.where(keep, a, pltpu.roll(b, 64, 1)),
            jnp.where(keep, pltpu.roll(a, 64, 1), b),
        )

    for c in vloads:
        c.wait()
    along_p = jnp.zeros((8, 128), F32)
    for i in range(64):
        along_p = jnp.where((lane & 63) == i, vxs[64 * gx + i], along_p)
    along_qp = [
        along_p + jnp.where(low, vys[16 * me + q], vys[16 * me + q + 8]) for q in range(8)
    ]

    def reciprocals(g, _):
        col = jnp.zeros((8, 128), F32)
        for i in range(8):
            col = jnp.where(sub == i, vzs[8 * g + i], col)
        rows = pl.ds(pl.multiple_of(8 * g, 8), 8)
        for q in range(8):
            recip[rows, 128 * q : 128 * (q + 1)] = 1.0 / (col + along_qp[q])
        return 0

    lax.fori_loop(0, N // 8, reciprocals, 0)

    loads[3].wait()
    row = lax.broadcasted_iota(jnp.int32, (N, N), 0)
    wanted = ((row & 63) >> 1) * 16 + (row >> 6) * 2 + (row & 1)
    order = (lax.broadcasted_iota(jnp.int32, (N, N), 1) == wanted).astype(F32).astype(BF16)
    izp[...] = dot(order, weights[3]).astype(BF16)

    my_block = pl.ds(pl.multiple_of(64 * gx, 64), 64)
    my_lines = pl.ds(pl.multiple_of(16 * me, 16), 16)

    def forward_x(k):
        p, n = FORWARD[k]
        arrived(xin.at[p : p + n], recv.at[0, k], f"x{k}")
        o = dot_t(xin[p : p + n].reshape(128 * n, N), weights[0]).reshape(n, 2, 64, N)
        for j in range(n):
            for t in range(4):
                a, b = exchange_halves(o[j, 0, :, 128 * t : 128 * (t + 1)], o[j, 1, :, 128 * t : 128 * (t + 1)])
                psend[2 * t, p + j] = a.astype(BF16)
                psend[2 * t + 1, p + j] = b.astype(BF16)
        for to, where in plane_peers:
            remote(psend.at[to, p : p + n], ybuf.at[p : p + n, my_block, :], 1, k, where)
        for j in range(p, p + n):
            ybuf[j, my_block, :] = psend[gx, j]

    to_gz = [lax.rem(gz + c, NZ) for c in range(NZ)]
    near = [[2 * x_lo + c, 2 * (1 - x_lo) + c] for c in range(2)]
    near_slab = [[slab_of(b) for b in pair] for pair in near]
    partner = 2 * x_lo + 1 - core

    def line_peers(half):
        for c in FAR_FIRST:
            for b, place in zip(near[half], near_slab[half]):
                yield to_gz[c] * NY + place, dev(gx, b, to_gz[c])
        yield gz * NY + near_slab[half][1], dev(gx, near[half][1], gz)
        if half == 0:
            yield gz * NY + slab_of(partner), dev(gx, partner, gz)

    def forward_y(k):
        p, n = FORWARD[k]
        arrived(psend.at[0 : NX - 1, p : p + n], recv.at[1, k], f"y{k}")
        o = dot(weights[1], jnp.concatenate([ybuf[j] for j in range(p, p + n)], axis=1))
        for j in range(n):
            yout[p + j] = o[:, 128 * j : 128 * (j + 1)].astype(BF16)

        for j in range(p, p + n):
            zbuf[me, j] = yout[j, my_lines, :]

    def send_lines(k, half):
        p, n = FORWARD[k]
        if (k, half) == (0, 0):
            @pl.when(gz < EARLY)
            def _():
                pl.semaphore_wait(ready, NY * (NZ - 1 - gz))

            @pl.when(gz >= EARLY)
            def _():
                pl.semaphore_wait(ready, 1)

            @pl.when(gz == 0)
            def _():
                for c in range(EARLY, NZ):
                    pl.semaphore_signal(ready, inc=1, device_id=dev(gx, gy, c), device_id_type=MESH)

        for place, where in line_peers(half):
            rows = pl.ds(pl.multiple_of(16 * place, 16), 16)
            remote(yout.at[p : p + n, rows, :], zbuf.at[me, p : p + n], 2, k, where)

    def to_z_rows(k):
        p, n = FORWARD[k]
        arrived(zbuf.at[0 : NZ * NY - 1, p : p + n], recv.at[2, k], f"z{k}")

        def some(g, _):
            for s in range(8):
                for j in range(p, p + n):
                    tile = zbuf[8 * g + s, j].astype(F32)
                    a, b = exchange_halves(tile[:8], tile[8:])
                    z = 16 * (8 * g + s) + 2 * j
                    zlines[pl.ds(z, 8, stride=PITCH), :] = a
                    zlines[pl.ds(z + 1, 8, stride=PITCH), :] = b
            return 0

        lax.fori_loop(0, 4, some, 0)

    def along_z():
        for h in range(4):
            d = jnp.concatenate(
                [zlines[PITCH * q : PITCH * q + N, :] for q in (2 * h, 2 * h + 1)], axis=1
            ).astype(BF16)
            c = dot(weights[2], d).astype(BF16).astype(F32)
            scaled[:, 256 * h : 256 * (h + 1)] = (c * recip[:, 256 * h : 256 * (h + 1)]).astype(BF16)

    def from_z_rows(k):
        p, n = INVERSE[k]
        for h in range(4):
            o = dot(izp[64 * p : 64 * (p + n), :], scaled[:, 256 * h : 256 * (h + 1)])
            for j in range(2):
                at = PITCH * (2 * h + j) + 64 * p
                olines[at : at + 64 * n, :] = o[:, 128 * j : 128 * (j + 1)]

        def some(g, _):
            for s in range(8):
                for j in range(p, p + n):
                    at = 64 * j + 2 * (8 * g + s)
                    a, b = exchange_halves(
                        olines[pl.ds(at, 8, stride=PITCH), :], olines[pl.ds(at + 1, 8, stride=PITCH), :]
                    )
                    zsend[8 * g + s, j] = jnp.concatenate([a, b], axis=0).astype(BF16)
            return 0

        lax.fori_loop(0, 4, some, 0)

        for half in range(2):
            for place, where in line_peers(half):
                remote(zsend.at[place, p : p + n], ybuf2.at[p : p + n, my_lines, :], 3, k, where)
        for j in range(p, p + n):
            ybuf2[j, my_lines, :] = zsend[me, j]

    def inverse_y(k):
        p, n = INVERSE[k]
        arrived(zsend.at[0 : NZ * NY - 1, p : p + n], recv.at[3, k], f"yi{k}")
        o = dot(weights[4], jnp.concatenate([ybuf2[j] for j in range(p, p + n)], axis=1))
        for j in range(n):
            yout2[p + j] = o[:, 128 * j : 128 * (j + 1)].astype(BF16)
        for to, where in plane_peers:
            rows = pl.ds(pl.multiple_of(64 * to, 64), 64)
            remote(yout2.at[p : p + n, rows, :], pbuf.at[gx, p : p + n], 4, k, where)
        for j in range(p, p + n):
            pbuf[gx, j] = yout2[j, my_block, :]

    def inverse_x(k):
        p, n = INVERSE[k]
        arrived(pbuf.at[0 : NX - 1, p : p + n], recv.at[4, k], f"xi{k}")
        for j in range(p, p + n):
            for t in range(4):
                a, b = exchange_halves(pbuf[2 * t, j].astype(F32), pbuf[2 * t + 1, j].astype(F32))
                xg[2 * j, :, 128 * t : 128 * (t + 1)] = a.astype(BF16)
                xg[2 * j + 1, :, 128 * t : 128 * (t + 1)] = b.astype(BF16)
        here = slice(2 * p, 2 * (p + n))
        o = dot_t(xg[here].reshape(128 * n, N), weights[5])
        xout[here] = o.astype(BF16).reshape(2 * n, 64, N)
        mine = pl.ds(16 * slab + 2 * p, 2 * n)
        for d in (2, 3, 1):
            to = lax.rem(gy + d, NY)
            columns = pl.ds(pl.multiple_of(128 * to, 128), 128)
            remote(xout.at[here, :, columns], out.at[mine], 5, 0, dev(gx, to, gz))
        out[mine] = xout[here, :, my_columns]

    loads[0].wait()
    loads[1].wait()
    for stage, *k in FORWARD_ORDER:
        {"x": forward_x, "y": forward_y, "z": send_lines}[stage](*k)
    for k in range(len(FORWARD)):
        to_z_rows(k)
    loads[2].wait()
    with jax.named_scope("c_z"):
        along_z()
    for k in range(len(INVERSE)):
        with jax.named_scope(f"c_from{k}"):
            from_z_rows(k)
    loads[4].wait()
    loads[5].wait()
    for stage, k in INVERSE_ORDER:
        (inverse_x if stage == "x" else inverse_y)(k)

    arrived(staged.at[0:48], recv.at[5, 0])
    arrived(staged.at[0:48], send.at[0])
    arrived(staged.at[0:48], send.at[5])
    arrived(psend.at[0 : NX - 1], send.at[1])
    arrived(psend.at[0 : NX - 1], send.at[4])
    arrived(zbuf.at[0 : NZ * NY - 1], send.at[2])
    arrived(zbuf.at[0 : NZ * NY - 1], send.at[3])


def on_device(source, *rest):
    pieces = pltpu.VMEM((NX, PAIRS, 64, 128), BF16)
    planes = pltpu.VMEM((PAIRS, N, 128), BF16)
    lines = pltpu.VMEM((NZ * NY, PAIRS, 16, 128), BF16)
    pencils = pltpu.VMEM((2 * PAIRS, 64, N), BF16)
    stages = max(len(FORWARD), len(INVERSE))
    return pl.pallas_call(
        kernel,
        out_shape=pltpu.VMEM(source.shape, BF16),
        in_specs=[pl.BlockSpec(memory_space=pl.ANY)] * 10,
        out_specs=pl.BlockSpec(memory_space=pltpu.VMEM),
        scratch_shapes=[
            pltpu.VMEM(source.shape, BF16),
            pltpu.VMEM((PAIRS, 2, 64, N), BF16),
            pieces,
            planes,
            planes,
            lines,
            pltpu.VMEM((9 * PITCH, 128), F32),
            pltpu.VMEM((N, 1024), F32),
            pltpu.VMEM((N, 1024), BF16),
            pltpu.VMEM((9 * PITCH, 128), F32),
            lines,
            planes,
            planes,
            pieces,
            pencils,
            pencils,
            pltpu.VMEM((6, N, N), BF16),
            pltpu.VMEM((N, N), BF16),
            pltpu.SMEM((N,), F32),
            pltpu.SMEM((N,), F32),
            pltpu.SMEM((N,), F32),
            pltpu.SemaphoreType.DMA((6, stages)),
            pltpu.SemaphoreType.DMA((6,)),
            pltpu.SemaphoreType.DMA((6,)),
            pltpu.SemaphoreType.DMA((3,)),
            pltpu.SemaphoreType.DMA,
            pltpu.SemaphoreType.REGULAR,
        ],
        compiler_params=pltpu.CompilerParams(
            collective_id=0, has_side_effects=True, vmem_limit_bytes=60 * 1024 * 1024
        ),
    )(source, *rest)


def solution(mesh):
    return jax.shard_map(
        on_device,
        mesh=mesh,
        in_specs=(P("gz", "gx", "gy"),) + (P(),) * 9,
        out_specs=P("gz", "gx", "gy"),
        check_vma=False,
    )
```

```python
import jax
import jax.numpy as jnp
from jax import lax
from jax.experimental import pallas as pl
from jax.experimental.pallas import tpu as pltpu
from jax.sharding import PartitionSpec as P

MESH = pl.DeviceIdType.MESH
F32 = jnp.float32
BF16 = jnp.bfloat16
NX, NY, NZ = 8, 4, 8
N = 512
PAIRS = 8
FORWARD = ((0, 1), (1, 1), (2, 2), (4, 2), (6, 2))
INVERSE = ((0, 1), (1, 2), (3, 2), (5, 1), (6, 1), (7, 1))
FORWARD_ORDER = (
    ("x", 0), ("x", 1), ("x", 2), ("y", 0), ("z", 0, 0), ("z", 0, 1), ("y", 1), ("z", 1, 0), ("z", 1, 1),
    ("x", 3), ("y", 2), ("z", 2, 0), ("z", 2, 1), ("x", 4), ("y", 3), ("z", 3, 0), ("y", 4), ("z", 4, 0),
    ("z", 3, 1), ("z", 4, 1),
)
INVERSE_ORDER = (
    ("y", 0), ("y", 1), ("x", 0), ("y", 2), ("x", 1), ("y", 3), ("y", 4), ("x", 2), ("y", 5), ("x", 3), ("x", 4), ("x", 5),
)
PITCH = N + 8
FAR_FIRST = (4, 3, 5, 2, 6, 1, 7)
PLANE_FAR_FIRST = ((2, 1), (1, 1), (3, 1), (2, 0), (0, 1), (1, 0), (3, 0))


def dot(a, b):
    return jnp.dot(a, b, preferred_element_type=F32)


def dot_t(a, b):
    return lax.dot_general(a, b, (((1,), (1,)), ((), ())), preferred_element_type=F32)


def kernel(
    src, fx, fy, fz, ix, iy, iz, vx, vy, vz, out,
    staged, xin, psend, ybuf, yout, zbuf, zlines, recip, scaled, olines, zsend, ybuf2, yout2, pbuf, xg, xout,
    weights, izp, vxs, vys, vzs, recv, send, wsem, vsem, ssem, ready,
):
    gx, gy, gz = lax.axis_index("gx"), lax.axis_index("gy"), lax.axis_index("gz")
    x_hi, x_lo, core = lax.rem(gx, 2), gy // 2, lax.rem(gy, 2)

    def xor(a, b):
        return a + b - 2 * a * b

    def slab_of(b):
        return 2 * xor(b // 2, x_hi) + lax.rem(b, 2)

    def same_slab(a):
        return 2 * xor(slab // 2, lax.rem(a, 2)) + core

    slab = slab_of(gy)
    me = gz * NY + slab

    def dev(a, b, c):
        return {"gx": a, "gy": b, "gz": c}

    plane_peers = []
    for d, h in PLANE_FAR_FIRST:
        to = 2 * lax.rem(gx // 2 + d, NX // 2) + (xor(x_hi, 1) if h else x_hi)
        plane_peers.append((to, dev(to, same_slab(to), gz)))

    def remote(s, d, stage, k, where):
        pltpu.make_async_remote_copy(
            src_ref=s, dst_ref=d, send_sem=send.at[stage], recv_sem=recv.at[stage, k],
            device_id=where, device_id_type=MESH,
        ).start()

    def arrived(ref, sem, name="end"):
        with jax.named_scope(f"w_{name}"):
            pltpu.make_async_copy(ref, ref, sem).wait()

    barrier = pltpu.get_barrier_semaphore()
    for _, where in plane_peers:
        pl.semaphore_signal(barrier, inc=1, device_id=where, device_id_type=MESH)
    for b in range(1, NY):
        pl.semaphore_signal(barrier, inc=1, device_id=dev(gx, lax.rem(gy + b, NY), gz), device_id_type=MESH)
    for c in range(1, NZ):
        @pl.when(c > gz)
        def _():
            for b in range(NY):
                pl.semaphore_signal(barrier, inc=1, device_id=dev(gx, b, c), device_id_type=MESH)

    stage_in = pltpu.make_async_copy(src, staged, ssem)
    stage_in.start()
    my_columns = pl.ds(pl.multiple_of(128 * gy, 128), 128)
    for k, (p, n) in enumerate(FORWARD):
        for j in range(p, p + n):
            pltpu.make_async_copy(
                src.at[pl.ds(16 * slab + 2 * j, 2)], xin.at[j, :, :, my_columns], recv.at[0, k]
            ).start()
    loads = [pltpu.make_async_copy(w, weights.at[i], wsem.at[i]) for i, w in enumerate((fx, fy, fz, iz, iy, ix))]
    for c in loads:
        c.start()
    vloads = [pltpu.make_async_copy(v, s, vsem.at[i]) for i, (v, s) in enumerate(((vx, vxs), (vy, vys), (vz, vzs)))]
    for c in vloads:
        c.start()

    with jax.named_scope("w_barrier"):
        pl.semaphore_wait(barrier, NX - 1 + NY - 1 + NY * gz)
    stage_in.wait()

    for k, (p, n) in enumerate(FORWARD):
        for to in (2 * (1 - x_lo), 2 * (1 - x_lo) + 1, 2 * x_lo + 1 - core):
            for j in range(p, p + n):
                remote(
                    staged.at[pl.ds(16 * slab_of(to) + 2 * j, 2)],
                    xin.at[j, :, :, my_columns],
                    0, k, dev(gx, to, gz),
                )

    for c in range(NZ - 1):
        @pl.when(c < gz)
        def _():
            for b in range(NY):
                pl.semaphore_signal(ready, inc=1, device_id=dev(gx, b, c), device_id_type=MESH)

    lane = lax.broadcasted_iota(jnp.int32, (8, 128), 1)
    sub = lax.broadcasted_iota(jnp.int32, (8, 128), 0)
    low = lane < 64

    def exchange_halves(a, b):
        keep = jnp.broadcast_to(lax.broadcasted_iota(jnp.int32, (1, 128), 1) < 64, a.shape)
        return (
            jnp.where(keep, a, pltpu.roll(b, 64, 1)),
            jnp.where(keep, pltpu.roll(a, 64, 1), b),
        )

    for c in vloads:
        c.wait()
    along_p = jnp.zeros((8, 128), F32)
    for i in range(64):
        along_p = jnp.where((lane & 63) == i, vxs[64 * gx + i], along_p)
    along_qp = [
        along_p + jnp.where(low, vys[16 * me + q], vys[16 * me + q + 8]) for q in range(8)
    ]

    def reciprocals(g, _):
        col = jnp.zeros((8, 128), F32)
        for i in range(8):
            col = jnp.where(sub == i, vzs[8 * g + i], col)
        rows = pl.ds(pl.multiple_of(8 * g, 8), 8)
        for q in range(8):
            recip[rows, 128 * q : 128 * (q + 1)] = 1.0 / (col + along_qp[q])
        return 0

    lax.fori_loop(0, N // 8, reciprocals, 0)

    loads[3].wait()
    row = lax.broadcasted_iota(jnp.int32, (N, N), 0)
    wanted = ((row & 63) >> 1) * 16 + (row >> 6) * 2 + (row & 1)
    order = (lax.broadcasted_iota(jnp.int32, (N, N), 1) == wanted).astype(F32).astype(BF16)
    izp[...] = dot(order, weights[3]).astype(BF16)

    my_block = pl.ds(pl.multiple_of(64 * gx, 64), 64)
    my_lines = pl.ds(pl.multiple_of(16 * me, 16), 16)

    def forward_x(k):
        p, n = FORWARD[k]
        arrived(xin.at[p : p + n], recv.at[0, k], f"x{k}")
        o = dot_t(xin[p : p + n].reshape(128 * n, N), weights[0]).reshape(n, 2, 64, N)
        for j in range(n):
            for t in range(4):
                a, b = exchange_halves(o[j, 0, :, 128 * t : 128 * (t + 1)], o[j, 1, :, 128 * t : 128 * (t + 1)])
                psend[2 * t, p + j] = a.astype(BF16)
                psend[2 * t + 1, p + j] = b.astype(BF16)
        for to, where in plane_peers:
            remote(psend.at[to, p : p + n], ybuf.at[p : p + n, my_block, :], 1, k, where)
        for j in range(p, p + n):
            ybuf[j, my_block, :] = psend[gx, j]

    to_gz = [lax.rem(gz + c, NZ) for c in range(NZ)]
    near = [[2 * x_lo + c, 2 * (1 - x_lo) + c] for c in range(2)]
    near_slab = [[slab_of(b) for b in pair] for pair in near]
    partner = 2 * x_lo + 1 - core

    def line_peers(half):
        for c in FAR_FIRST:
            for b, place in zip(near[half], near_slab[half]):
                yield to_gz[c] * NY + place, dev(gx, b, to_gz[c])
        yield gz * NY + near_slab[half][1], dev(gx, near[half][1], gz)
        if half == 0:
            yield gz * NY + slab_of(partner), dev(gx, partner, gz)

    def forward_y(k):
        p, n = FORWARD[k]
        arrived(psend.at[0 : NX - 1, p : p + n], recv.at[1, k], f"y{k}")
        o = dot(weights[1], jnp.concatenate([ybuf[j] for j in range(p, p + n)], axis=1))
        for j in range(n):
            yout[p + j] = o[:, 128 * j : 128 * (j + 1)].astype(BF16)

        for j in range(p, p + n):
            zbuf[me, j] = yout[j, my_lines, :]

    def send_lines(k, half):
        p, n = FORWARD[k]
        if (k, half) == (0, 0):
            @pl.when(gz < NZ - 1)
            def _():
                pl.semaphore_wait(ready, NY * (NZ - 1 - gz))

        for place, where in line_peers(half):
            rows = pl.ds(pl.multiple_of(16 * place, 16), 16)
            remote(yout.at[p : p + n, rows, :], zbuf.at[me, p : p + n], 2, k, where)

    def to_z_rows(k):
        p, n = FORWARD[k]
        arrived(zbuf.at[0 : NZ * NY - 1, p : p + n], recv.at[2, k], f"z{k}")

        def some(g, _):
            for s in range(8):
                for j in range(p, p + n):
                    tile = zbuf[8 * g + s, j].astype(F32)
                    a, b = exchange_halves(tile[:8], tile[8:])
                    z = 16 * (8 * g + s) + 2 * j
                    zlines[pl.ds(z, 8, stride=PITCH), :] = a
                    zlines[pl.ds(z + 1, 8, stride=PITCH), :] = b
            return 0

        lax.fori_loop(0, 4, some, 0)

    def along_z():
        for h in range(4):
            d = jnp.concatenate(
                [zlines[PITCH * q : PITCH * q + N, :] for q in (2 * h, 2 * h + 1)], axis=1
            ).astype(BF16)
            c = dot(weights[2], d).astype(BF16).astype(F32)
            scaled[:, 256 * h : 256 * (h + 1)] = (c * recip[:, 256 * h : 256 * (h + 1)]).astype(BF16)

    def from_z_rows(k):
        p, n = INVERSE[k]
        for h in range(4):
            o = dot(izp[64 * p : 64 * (p + n), :], scaled[:, 256 * h : 256 * (h + 1)])
            for j in range(2):
                at = PITCH * (2 * h + j) + 64 * p
                olines[at : at + 64 * n, :] = o[:, 128 * j : 128 * (j + 1)]

        def some(g, _):
            for s in range(8):
                for j in range(p, p + n):
                    at = 64 * j + 2 * (8 * g + s)
                    a, b = exchange_halves(
                        olines[pl.ds(at, 8, stride=PITCH), :], olines[pl.ds(at + 1, 8, stride=PITCH), :]
                    )
                    zsend[8 * g + s, j] = jnp.concatenate([a, b], axis=0).astype(BF16)
            return 0

        lax.fori_loop(0, 4, some, 0)

        for half in range(2):
            for place, where in line_peers(half):
                remote(zsend.at[place, p : p + n], ybuf2.at[p : p + n, my_lines, :], 3, k, where)
        for j in range(p, p + n):
            ybuf2[j, my_lines, :] = zsend[me, j]

    def inverse_y(k):
        p, n = INVERSE[k]
        arrived(zsend.at[0 : NZ * NY - 1, p : p + n], recv.at[3, k], f"yi{k}")
        o = dot(weights[4], jnp.concatenate([ybuf2[j] for j in range(p, p + n)], axis=1))
        for j in range(n):
            yout2[p + j] = o[:, 128 * j : 128 * (j + 1)].astype(BF16)
        for to, where in plane_peers:
            rows = pl.ds(pl.multiple_of(64 * to, 64), 64)
            remote(yout2.at[p : p + n, rows, :], pbuf.at[gx, p : p + n], 4, k, where)
        for j in range(p, p + n):
            pbuf[gx, j] = yout2[j, my_block, :]

    def inverse_x(k):
        p, n = INVERSE[k]
        arrived(pbuf.at[0 : NX - 1, p : p + n], recv.at[4, k], f"xi{k}")
        for j in range(p, p + n):
            for t in range(4):
                a, b = exchange_halves(pbuf[2 * t, j].astype(F32), pbuf[2 * t + 1, j].astype(F32))
                xg[2 * j, :, 128 * t : 128 * (t + 1)] = a.astype(BF16)
                xg[2 * j + 1, :, 128 * t : 128 * (t + 1)] = b.astype(BF16)
        here = slice(2 * p, 2 * (p + n))
        o = dot_t(xg[here].reshape(128 * n, N), weights[5])
        xout[here] = o.astype(BF16).reshape(2 * n, 64, N)
        mine = pl.ds(16 * slab + 2 * p, 2 * n)
        for to in (2 * (1 - x_lo), 2 * (1 - x_lo) + 1, 2 * x_lo + 1 - core):
            columns = pl.ds(pl.multiple_of(128 * to, 128), 128)
            remote(xout.at[here, :, columns], out.at[mine], 5, 0, dev(gx, to, gz))
        out[mine] = xout[here, :, my_columns]

    loads[0].wait()
    loads[1].wait()
    for stage, *k in FORWARD_ORDER:
        {"x": forward_x, "y": forward_y, "z": send_lines}[stage](*k)
    for k in range(len(FORWARD)):
        to_z_rows(k)
    loads[2].wait()
    with jax.named_scope("c_z"):
        along_z()
    for k in range(len(INVERSE)):
        with jax.named_scope(f"c_from{k}"):
            from_z_rows(k)
    loads[4].wait()
    loads[5].wait()
    for stage, k in INVERSE_ORDER:
        (inverse_x if stage == "x" else inverse_y)(k)

    arrived(staged.at[0:48], recv.at[5, 0])
    arrived(staged.at[0:48], send.at[0])
    arrived(staged.at[0:48], send.at[5])
    arrived(psend.at[0 : NX - 1], send.at[1])
    arrived(psend.at[0 : NX - 1], send.at[4])
    arrived(zbuf.at[0 : NZ * NY - 1], send.at[2])
    arrived(zbuf.at[0 : NZ * NY - 1], send.at[3])


def on_device(source, *rest):
    pieces = pltpu.VMEM((NX, PAIRS, 64, 128), BF16)
    planes = pltpu.VMEM((PAIRS, N, 128), BF16)
    lines = pltpu.VMEM((NZ * NY, PAIRS, 16, 128), BF16)
    pencils = pltpu.VMEM((2 * PAIRS, 64, N), BF16)
    stages = max(len(FORWARD), len(INVERSE))
    return pl.pallas_call(
        kernel,
        out_shape=pltpu.VMEM(source.shape, BF16),
        in_specs=[pl.BlockSpec(memory_space=pl.ANY)] * 10,
        out_specs=pl.BlockSpec(memory_space=pltpu.VMEM),
        scratch_shapes=[
            pltpu.VMEM(source.shape, BF16),
            pltpu.VMEM((PAIRS, 2, 64, N), BF16),
            pieces,
            planes,
            planes,
            lines,
            pltpu.VMEM((8 * PITCH, 128), F32),
            pltpu.VMEM((N, 1024), F32),
            pltpu.VMEM((N, 1024), BF16),
            pltpu.VMEM((8 * PITCH, 128), F32),
            lines,
            planes,
            planes,
            pieces,
            pencils,
            pencils,
            pltpu.VMEM((6, N, N), BF16),
            pltpu.VMEM((N, N), BF16),
            pltpu.SMEM((N,), F32),
            pltpu.SMEM((N,), F32),
            pltpu.SMEM((N,), F32),
            pltpu.SemaphoreType.DMA((6, stages)),
            pltpu.SemaphoreType.DMA((6,)),
            pltpu.SemaphoreType.DMA((6,)),
            pltpu.SemaphoreType.DMA((3,)),
            pltpu.SemaphoreType.DMA,
            pltpu.SemaphoreType.REGULAR,
        ],
        compiler_params=pltpu.CompilerParams(
            collective_id=0, has_side_effects=True, vmem_limit_bytes=60 * 1024 * 1024
        ),
    )(source, *rest)


def solution(mesh):
    return jax.shard_map(
        on_device,
        mesh=mesh,
        in_specs=(P("gz", "gx", "gy"),) + (P(),) * 9,
        out_specs=P("gz", "gx", "gy"),
        check_vma=False,
    )
```
